32 devices in a mesh: row: 8 (over z, core), col: 4 (over y, x).
Axes of the slice: x: 2, y: 2, z: 4, core: 2. Of those that a mesh axis runs over, the one named last changes fastest.
Arguments:
- images: bfloat16 [512, 12, 12, 272], P(('row', 'col')), may hold values from -20 to 20
- expand_weight: bfloat16 [2, 272, 1632], replicated, may hold values from -0.375 to 0.375
- depth_kernel: float32 [2, 25, 1632], replicated, may hold values from -1.25 to 1.25
- squeeze_weight: float32 [2, 1632, 68], replicated, may hold values from -0.15625 to 0.15625
- squeeze_bias: float32 [2, 68], replicated, may hold values from -3 to 3
- excite_weight: float32 [2, 68, 1632], replicated, may hold values from -0.75 to 0.75
- excite_bias: float32 [2, 1632], replicated, may hold values from -4 to 4
- project_weight: bfloat16 [2, 1632, 272], replicated, may hold values from -0.15625 to 0.15625
- mid_gain: float32 [2, 2, 1632], replicated, may hold values from 0.5 to 1.5
- mid_bias: float32 [2, 2, 1632], replicated, may hold values from -3 to 3
- out_gain: float32 [2, 272], replicated, may hold values from 0.5 to 1.5
- out_bias: float32 [2, 272], replicated, may hold values from -3 to 3
- mid_mean: float32 [2, 2, 1632], replicated, may hold values from -4 to 4
- mid_var: float32 [2, 2, 1632], replicated, may hold values from 0.05 to 20
- out_mean: float32 [2, 272], replicated, may hold values from -4 to 4
- out_var: float32 [2, 272], replicated, may hold values from 0.05 to 20
Outputs:
- block_output: bfloat16 [512, 12, 12, 272], P(('row', 'col'))
- mid_mean_new: float32 [2, 2, 1632], replicated
- mid_var_new: float32 [2, 2, 1632], replicated
- out_mean_new: float32 [2, 272], replicated
- out_var_new: float32 [2, 272], replicated
The draws below stay inside these ranges and needn't reach their ends.
All inputs are finite; a program needn't handle non-finite values.
Results may differ from the reference program's by a relative error of at most 0.0049.
The reference program's roundings to bfloat16 on the way (of `active` and `scaled`) count: a program that leaves them out, or rounds other values in their place, can miss the bound.
Values sent between devices are 32-bit elements; how exact they have to be, the bound alone decides.
A program may use at most 128 MiB of HBM per device.

```python
import math
import jax
import jax.numpy as jnp
from jax import lax

OUT = 272
MID = 1632
SQZ = 68
KERN = 5
SIDE = 12
LAYERS = 2
BATCH = 512


def draw_images(key, part):
    subkeys = jax.random.split(jax.random.fold_in(key, 11), 2)
    rising = 1.0 + 2.0 * jnp.arange(BATCH, dtype=jnp.float32) / max(BATCH - 1, 1)
    offset = 0.5 * jax.random.truncated_normal(subkeys[0], -4.0, 4.0, (OUT,), jnp.float32)
    noise_draw = jax.random.truncated_normal(subkeys[1], -4.0, 4.0, (BATCH, SIDE, SIDE, OUT), jnp.float32)
    return (noise_draw * rising[:, None, None, None] + offset).astype(jnp.bfloat16)


def scatter_about(key, extent, deviation, most, held_as=jnp.bfloat16):
    array = jax.random.normal(key, extent, jnp.float32) * deviation
    return jnp.minimum(jnp.maximum(array, -most), most).astype(held_as)


def setup_inputs(seed: int = 0) -> dict:
    streams_of = jax.random.split(jax.random.key(seed), 17)
    return {
        "images": draw_images(jax.random.fold_in(streams_of[16], 71), 0),
        "expand_weight": scatter_about(streams_of[1], (LAYERS, OUT, MID), OUT ** -0.5, 0.375),
        "depth_kernel": scatter_about(streams_of[2], (LAYERS, KERN * KERN, MID), (KERN * KERN) ** -0.5, 1.25, jnp.float32),
        "squeeze_weight": scatter_about(streams_of[3], (LAYERS, MID, SQZ), MID ** -0.5, 0.15625, jnp.float32),
        "squeeze_bias": scatter_about(streams_of[4], (LAYERS, SQZ), 0.5, 3.0, jnp.float32),
        "excite_weight": scatter_about(streams_of[5], (LAYERS, SQZ, MID), SQZ ** -0.5, 0.75, jnp.float32),
        "excite_bias": scatter_about(streams_of[6], (LAYERS, MID), 1.0, 4.0, jnp.float32),
        "project_weight": scatter_about(streams_of[7], (LAYERS, MID, OUT), MID ** -0.5, 0.15625),
        "mid_gain": jnp.clip(1.0 + 0.1 * jax.random.normal(streams_of[8], (LAYERS, 2, MID), jnp.float32), 0.5, 1.5),
        "mid_bias": scatter_about(streams_of[9], (LAYERS, 2, MID), 0.5, 3.0, jnp.float32),
        "out_gain": jnp.clip(1.0 + 0.1 * jax.random.normal(streams_of[10], (LAYERS, OUT), jnp.float32), 0.5, 1.5),
        "out_bias": scatter_about(streams_of[11], (LAYERS, OUT), 0.5, 3.0, jnp.float32),
        "mid_mean": scatter_about(streams_of[12], (LAYERS, 2, MID), 1.0, 4.0, jnp.float32),
        "mid_var": jnp.clip(jnp.exp(jax.random.uniform(streams_of[13], (LAYERS, 2, MID), jnp.float32, math.log(0.05), math.log(20.0))), 0.05, 20.0),
        "out_mean": scatter_about(streams_of[14], (LAYERS, OUT), 1.0, 4.0, jnp.float32),
        "out_var": jnp.clip(jnp.exp(jax.random.uniform(streams_of[15], (LAYERS, OUT), jnp.float32, math.log(0.05), math.log(20.0))), 0.05, 20.0),
    }


EPSILON = 0.001
RATIO_MAX = 3.0
SHIFT_MAX = 5.0
MOMENTUM = 0.01

def coefficients(first_sum, second_sum, row_count, run_mean, run_var, gain, bias):
    offset = first_sum / row_count
    batch_var = second_sum / row_count - offset * offset
    batch_mean = run_mean + offset
    batch_sigma = jnp.sqrt(batch_var + EPSILON)
    run_sigma = jnp.sqrt(run_var + EPSILON)
    scale_ratio = jnp.clip(batch_sigma / run_sigma, 1.0 / RATIO_MAX, RATIO_MAX)
    shift_clip = jnp.clip(offset / run_sigma, -SHIFT_MAX, SHIFT_MAX)
    gain_scale = gain * scale_ratio / batch_sigma
    gain_shift = bias + gain * shift_clip - batch_mean * gain_scale
    new_mean = run_mean + MOMENTUM * offset
    new_var = run_var + MOMENTUM * (batch_var - run_var)
    return (gain_scale, gain_shift, new_mean, new_var)

def moments(values, run_mean):
    centered = values - run_mean
    return (lax.optimization_barrier(jnp.sum(centered, axis=(0, 1, 2))), lax.optimization_barrier(jnp.sum(centered * centered, axis=(0, 1, 2))))

def project_rows(images, matrix):
    leading = images.shape[:3]
    flat_rows = images.reshape(-1, images.shape[3])
    product = jnp.dot(flat_rows, matrix, preferred_element_type=jnp.float32)
    return product.reshape(leading + (matrix.shape[1],))

def depthwise(active, kernel):
    reach = KERN // 2
    side_len = active.shape[1]
    padded = jnp.pad(active, ((0, 0), (reach, reach), (reach, reach), (0, 0)))
    running_total = jnp.zeros(active.shape, jnp.float32)
    for row_step in range(KERN):
        for col_step in range(KERN):
            window = padded[:, row_step:row_step + side_len, col_step:col_step + side_len, :]
            running_total = running_total + window * kernel[row_step * KERN + col_step]
    return running_total

def excite(lifted, reduce_w, reduce_b, grow_w, grow_b):
    pooled = lax.optimization_barrier(jnp.mean(lifted, axis=(1, 2)))
    squeezed = jax.nn.silu(jnp.dot(pooled, reduce_w, precision=lax.Precision.HIGHEST) + reduce_b)
    se_gate = jax.nn.sigmoid(jnp.dot(squeezed, grow_w, precision=lax.Precision.HIGHEST) + grow_b)
    return (lifted * se_gate[:, None, None, :]).astype(jnp.bfloat16)

def through(group, params, scales, norm_depth):
    expand_w, kernel, reduce_w, reduce_b, grow_w, grow_b, project_w = params
    expanded = project_rows(group, expand_w)
    if norm_depth == 0:
        return expanded
    active = jax.nn.silu(expanded * scales[0][0] + scales[0][1]).astype(jnp.bfloat16)
    spread = depthwise(active, kernel)
    if norm_depth == 1:
        return spread
    lifted = jax.nn.silu(spread * scales[1][0] + scales[1][1])
    scaled = excite(lifted, reduce_w, reduce_b, grow_w, grow_b)
    projected = project_rows(scaled, project_w)
    if norm_depth == 2:
        return projected
    return (group.astype(jnp.float32) + projected * scales[2][0] + scales[2][1]).astype(jnp.bfloat16)

def reference(images, expand_weight, depth_kernel, squeeze_weight, squeeze_bias, excite_weight, excite_bias, project_weight, mid_gain, mid_bias, out_gain, out_bias, mid_mean, mid_var, out_mean, out_var):
    row_count = float(BATCH * SIDE * SIDE)
    block = math.gcd(BATCH, 32)
    current = images
    mean_layers, var_layers, out_means, out_vars = ([], [], [], [])
    for layer_index in range(LAYERS):
        params = (expand_weight[layer_index], depth_kernel[layer_index], squeeze_weight[layer_index], squeeze_bias[layer_index], excite_weight[layer_index], excite_bias[layer_index], project_weight[layer_index])
        norm_stats = [(mid_mean[layer_index, 0], mid_var[layer_index, 0], mid_gain[layer_index, 0], mid_bias[layer_index, 0]), (mid_mean[layer_index, 1], mid_var[layer_index, 1], mid_gain[layer_index, 1], mid_bias[layer_index, 1]), (out_mean[layer_index], out_var[layer_index], out_gain[layer_index], out_bias[layer_index])]
        grouped = current.reshape((BATCH // block, block) + current.shape[1:])
        scales = []
        new_stats = []
        for norm_depth in range(3):
            run_mean, run_var, gain, bias = norm_stats[norm_depth]
            first_parts, second_parts = lax.map(lambda group: moments(through(group, params, scales, norm_depth), run_mean), grouped)
            gain_scale, gain_shift, new_mean, new_var = coefficients(lax.optimization_barrier(jnp.sum(first_parts, axis=0)), lax.optimization_barrier(jnp.sum(second_parts, axis=0)), row_count, run_mean, run_var, gain, bias)
            scales.append((gain_scale, gain_shift))
            new_stats.append((new_mean, new_var))
        current = lax.map(lambda group: through(group, params, scales, 3), grouped).reshape(current.shape)
        mean_layers.append(jnp.stack([new_stats[0][0], new_stats[1][0]]))
        var_layers.append(jnp.stack([new_stats[0][1], new_stats[1][1]]))
        out_means.append(new_stats[2][0])
        out_vars.append(new_stats[2][1])
    return (current, jnp.stack(mean_layers), jnp.stack(var_layers), jnp.stack(out_means), jnp.stack(out_vars))
```

```python
import functools

import jax
import jax.numpy as jnp
from jax import lax
from jax.experimental import pallas as pl
from jax.experimental.pallas import tpu as pltpu
from jax.sharding import PartitionSpec as P

KERN = 5
REACH = KERN // 2
LANES = 128
WIDE = 2 * LANES

EPSILON = 0.001
RATIO_MAX = 3.0
SHIFT_MAX = 5.0
MOMENTUM = 0.01

VMEM_BYTES = 60 * 1024 * 1024


def coefficients(first_sum, second_sum, row_count, run_mean, run_var, gain, bias):
    offset = first_sum / row_count
    batch_var = second_sum / row_count - offset * offset
    batch_mean = run_mean + offset
    batch_sigma = jnp.sqrt(batch_var + EPSILON)
    run_sigma = jnp.sqrt(run_var + EPSILON)
    scale_ratio = jnp.clip(batch_sigma / run_sigma, 1.0 / RATIO_MAX, RATIO_MAX)
    shift_clip = jnp.clip(offset / run_sigma, -SHIFT_MAX, SHIFT_MAX)
    gain_scale = gain * scale_ratio / batch_sigma
    gain_shift = bias + gain * shift_clip - batch_mean * gain_scale
    new_mean = run_mean + MOMENTUM * offset
    new_var = run_var + MOMENTUM * (batch_var - run_var)
    return (gain_scale, gain_shift, new_mean, new_var)


def half_silu(half_value):
    return half_value + half_value * jnp.tanh(half_value)


def fold_rows(values):
    return jnp.sum(values.reshape(-1, 8, values.shape[-1]), axis=0)


def exchange_kernel(n_row, n_col, x_ref, o_ref, buf_row, part, buf_col, s_row, r_row, s_col, r_col):
    row = lax.axis_index("row")
    col = lax.axis_index("col")
    row_peers = [lax.rem(row + k, n_row) for k in range(1, n_row)]
    col_peers = [lax.rem(col + k, n_col) for k in range(1, n_col)]
    mesh_id = pl.DeviceIdType.MESH
    barrier = pltpu.get_barrier_semaphore()
    for peer in row_peers:
        pl.semaphore_signal(barrier, inc=1, device_id=(peer, col), device_id_type=mesh_id)
    for peer in col_peers:
        pl.semaphore_signal(barrier, inc=1, device_id=(row, peer), device_id_type=mesh_id)
    pl.semaphore_wait(barrier, len(row_peers) + len(col_peers))

    copies = []
    for k, peer in enumerate(row_peers):
        copy = pltpu.make_async_remote_copy(
            src_ref=x_ref,
            dst_ref=buf_row.at[row],
            send_sem=s_row.at[k],
            recv_sem=r_row.at[k],
            device_id=(peer, col),
            device_id_type=mesh_id,
        )
        copy.start()
        copies.append(copy)
    buf_row[row] = x_ref[...]
    for copy in copies:
        copy.wait()
    total = buf_row[0]
    for k in range(1, n_row):
        total = total + buf_row[k]
    part[...] = total
    copies = []
    for k, peer in enumerate(col_peers):
        copy = pltpu.make_async_remote_copy(
            src_ref=part,
            dst_ref=buf_col.at[col],
            send_sem=s_col.at[k],
            recv_sem=r_col.at[k],
            device_id=(row, peer),
            device_id_type=mesh_id,
        )
        copy.start()
        copies.append(copy)
    buf_col[col] = total
    for copy in copies:
        copy.wait()
    total = buf_col[0]
    for k in range(1, n_col):
        total = total + buf_col[k]
    o_ref[...] = total


def all_sum(stats, n_row, n_col, collective_id):
    shape = stats.shape
    vmem = pl.BlockSpec(memory_space=pltpu.VMEM)
    return pl.pallas_call(
        functools.partial(exchange_kernel, n_row, n_col),
        out_shape=jax.ShapeDtypeStruct(shape, jnp.float32),
        in_specs=[vmem],
        out_specs=vmem,
        scratch_shapes=[
            pltpu.VMEM((n_row,) + shape, jnp.float32),
            pltpu.VMEM(shape, jnp.float32),
            pltpu.VMEM((n_col,) + shape, jnp.float32),
            pltpu.SemaphoreType.DMA((n_row - 1,)),
            pltpu.SemaphoreType.DMA((n_row - 1,)),
            pltpu.SemaphoreType.DMA((n_col - 1,)),
            pltpu.SemaphoreType.DMA((n_col - 1,)),
        ],
        compiler_params=pltpu.CompilerParams(collective_id=collective_id, has_side_effects=True),
    )(stats)


def expand_stats_kernel(chunk, x_ref, w_ref, mean_ref, stats_ref):
    mean = mean_ref[0, 0:1, :]
    weight = w_ref[0]

    def body(step, carry):
        rows = pl.ds(pl.multiple_of(step * chunk, chunk), chunk)
        y = jnp.dot(x_ref[rows, :], weight, preferred_element_type=jnp.float32)
        centered = y - mean
        return carry[0] + fold_rows(centered), carry[1] + fold_rows(centered * centered)

    zero = jnp.zeros((8, weight.shape[1]), jnp.float32)
    first, second = lax.fori_loop(0, x_ref.shape[0] // chunk, body, (zero, zero))
    stats_ref[0:1, :] = jnp.sum(first, axis=0, keepdims=True)
    stats_ref[1:2, :] = jnp.sum(second, axis=0, keepdims=True)


def residual_kernel(
    layer, chunk, row_count, x_ref, p_ref, s_ref, m_ref, v_ref, g_ref, b_ref, w_ref, mean_ref,
    cur_ref, stats_ref, nm_ref, nv_ref,
):
    @pl.when(pl.program_id(0) == 0)
    def _():
        pick = slice(layer, layer + 1)
        scale, shift, new_mean, new_var = coefficients(
            s_ref[0:1, :], s_ref[1:2, :], row_count,
            m_ref[pick, :], v_ref[pick, :], g_ref[pick, :], b_ref[pick, :],
        )
        nm_ref[...] = new_mean
        nv_ref[...] = new_var

        def body(step, carry):
            rows = pl.ds(pl.multiple_of(step * chunk, chunk), chunk)
            cur_ref[rows, :] = (
                x_ref[rows, :].astype(jnp.float32) + p_ref[rows, :] * scale + shift
            ).astype(jnp.bfloat16)
            return carry

        lax.fori_loop(0, x_ref.shape[0] // chunk, body, 0)

    expand_stats_kernel(chunk, cur_ref, w_ref, mean_ref, stats_ref)


def spread_kernel(
    side, batch, row_count, blocks, x_ref, w_ref, dk_ref, sums_ref, mean_ref, var_ref, gain_ref, bias_ref,
    spread_ref, stats_ref, nm_ref, nv_ref, act, taps,
):
    chunk = side * batch
    scale, shift, new_mean, new_var = coefficients(
        sums_ref[0:1, :], sums_ref[1:2, :], row_count,
        mean_ref[0, 0:1, :], var_ref[0, 0:1, :], gain_ref[0, 0:1, :], bias_ref[0, 0:1, :],
    )
    nm_ref[...] = new_mean
    nv_ref[...] = new_var
    half_scale, half_shift = 0.5 * scale, 0.5 * shift
    weight = w_ref[0]

    def activate(step, carry):
        rows = pl.ds(pl.multiple_of(step * chunk, chunk), chunk)
        y = jnp.dot(x_ref[rows, :], weight, preferred_element_type=jnp.float32)
        active = half_silu(y * half_scale + half_shift).astype(jnp.bfloat16).astype(jnp.float32)
        for half in range(2):
            act[half, step] = active[:, half * LANES : (half + 1) * LANES].reshape(side, batch, LANES)
        return carry

    lax.fori_loop(0, side, activate, 0)

    def half_block(half, carry):
        lanes = pl.ds(pl.multiple_of(half * LANES, LANES), LANES)
        for tap in range(KERN * KERN):
            taps[tap] = jnp.broadcast_to(dk_ref[0, tap : tap + 1, lanes], (8, LANES))
        mean = jnp.broadcast_to(mean_ref[0, 1:2, lanes], (8, LANES))

        def row(h, steps, sums):
            first, second = sums
            for sub in range(batch // 8):
                total = [None] * side
                for dy in steps:
                    line = [act[half, h + dy - REACH, w, sub * 8 : sub * 8 + 8, :] for w in range(side)]
                    for dx in range(KERN):
                        tap = taps[dy * KERN + dx]
                        for w in range(side):
                            source = w + dx - REACH
                            if 0 <= source < side:
                                term = line[source] * tap
                                total[w] = term if total[w] is None else total[w] + term
                for w in range(side):
                    start = pl.multiple_of((h * side + w) * batch + sub * 8, 8)
                    spread_ref[half, pl.ds(start, 8), :] = total[w]
                    centered = total[w] - mean
                    first = first + centered
                    second = second + centered * centered
            return first, second

        zero = jnp.zeros((8, LANES), jnp.float32)
        sums = (zero, zero)
        for h in range(REACH):
            sums = row(h, range(REACH - h, KERN), sums)
        sums = lax.fori_loop(REACH, side - REACH, lambda h, c: row(h, range(KERN), c), sums)
        for h in range(side - REACH, side):
            sums = row(h, range(0, side - h + REACH), sums)
        stats_ref[0:1, lanes] = jnp.sum(sums[0], axis=0, keepdims=True)
        stats_ref[1:2, lanes] = jnp.sum(sums[1], axis=0, keepdims=True)
        return carry

    halves = jnp.minimum(2, blocks - 2 * pl.program_id(0))
    lax.fori_loop(0, halves, half_block, 0)


def lift_kernel(
    layer, side, batch, row_count, mid, v_ref, sums_ref, mean_ref, var_ref, gain_ref, bias_ref,
    sw_ref, sb_ref, ew_ref, eb_ref, pw_ref, om_ref, proj_ref, stats_ref, nm_ref, nv_ref,
    lifted, pooled, gate, scaled,
):
    chunk = side * batch
    block = pl.program_id(0)
    blocks = pl.num_programs(0)
    scale, shift, new_mean, new_var = coefficients(
        sums_ref[0:1, :], sums_ref[1:2, :], row_count,
        mean_ref[0, 1:2, :], var_ref[0, 1:2, :], gain_ref[0, 1:2, :], bias_ref[0, 1:2, :],
    )
    nm_ref[...] = new_mean
    nv_ref[...] = new_var
    half_scale, half_shift = 0.5 * scale, 0.5 * shift

    def lift(step, total):
        rows = pl.ds(pl.multiple_of(step * chunk, chunk), chunk)
        value = half_silu(v_ref[0, rows, :] * half_scale + half_shift)
        lifted[block, rows, :] = value
        return total + jnp.sum(value.reshape(side, batch, LANES), axis=0)

    total = lax.fori_loop(0, side, lift, jnp.zeros((batch, LANES), jnp.float32))
    pooled[:, pl.ds(pl.multiple_of(block * LANES, LANES), LANES)] = total / float(side * side)

    @pl.when(block == blocks - 1)
    def _():
        pick = slice(layer, layer + 1)
        squeezed = jnp.dot(
            pooled[:, :mid], sw_ref[0], precision=lax.Precision.HIGHEST, preferred_element_type=jnp.float32
        )
        squeezed = half_silu(0.5 * (squeezed + sb_ref[pick, :]))
        grown = jnp.dot(
            squeezed, ew_ref[0], precision=lax.Precision.HIGHEST, preferred_element_type=jnp.float32
        )
        gate[:, :mid] = 0.5 + 0.5 * jnp.tanh(0.5 * (grown + eb_ref[pick, :]))
        out_mean = om_ref[pick, :]

        def project(step, sums):
            rows = pl.ds(pl.multiple_of(step * chunk, chunk), chunk)
            for index in range(pl.cdiv(mid, LANES)):
                start = index * LANES
                stop = min(mid, start + LANES)
                value = lifted[index, rows, :].reshape(side, batch, LANES) * gate[:, start : start + LANES]
                value = value.astype(jnp.bfloat16).reshape(chunk, LANES)
                scaled[:, start:stop] = value[:, : stop - start]
            product = jnp.dot(scaled[...], pw_ref[0], preferred_element_type=jnp.float32)
            proj_ref[rows, :] = product
            centered = product - out_mean
            return sums[0] + fold_rows(centered), sums[1] + fold_rows(centered * centered)

        zero = jnp.zeros((8, proj_ref.shape[1]), jnp.float32)
        first, second = lax.fori_loop(0, side, project, (zero, zero))
        stats_ref[0:1, :] = jnp.sum(first, axis=0, keepdims=True)
        stats_ref[1:2, :] = jnp.sum(second, axis=0, keepdims=True)


def whole(shape):
    return pl.BlockSpec(shape, lambda j: (0,) * len(shape))


def of_layer(shape, layer):
    return pl.BlockSpec((1,) + shape[1:], lambda j: (layer,) + (0,) * (len(shape) - 1))


def columns(rows, width):
    return pl.BlockSpec((rows, width), lambda j: (0, j))


def layer_columns(rows, width, layer):
    return pl.BlockSpec((1, rows, width), lambda j: (layer, 0, j))


def f32(*shape):
    return jax.ShapeDtypeStruct(shape, jnp.float32)


PARAMS = pltpu.CompilerParams(vmem_limit_bytes=VMEM_BYTES, dimension_semantics=("arbitrary",))


def per_device(n_row, n_col, *args):
    (
        images, expand_weight, depth_kernel, squeeze_weight, squeeze_bias, excite_weight, excite_bias,
        project_weight, mid_gain, mid_bias, out_gain, out_bias, mid_mean, mid_var, out_mean, out_var,
    ) = args
    batch, side, _, out = images.shape
    layers, _, mid = expand_weight.shape
    squeeze = squeeze_weight.shape[2]
    rows = side * side * batch
    chunk = side * batch
    row_count = float(rows * n_row * n_col)
    wide_steps = pl.cdiv(mid, WIDE)
    blocks = pl.cdiv(mid, LANES)
    taps_count = depth_kernel.shape[1]

    current = images.reshape(batch, side * side, out).transpose(1, 0, 2).reshape(rows, out)
    projected = None
    out_sums = None
    means, variances, out_means, out_vars = [], [], [], []
    for layer in range(layers):
        wide_params = [layer_columns(2, WIDE, layer)] * 4
        weight_spec = layer_columns(out, WIDE, layer)
        if layer == 0:
            stats = pl.pallas_call(
                functools.partial(expand_stats_kernel, chunk),
                grid=(wide_steps,),
                in_specs=[whole((rows, out)), weight_spec, wide_params[0]],
                out_specs=columns(2, WIDE),
                out_shape=f32(2, mid),
                compiler_params=PARAMS,
            )(current, expand_weight, mid_mean)
        else:
            current, stats, new_mean, new_var = pl.pallas_call(
                functools.partial(residual_kernel, layer - 1, chunk, row_count),
                grid=(wide_steps,),
                in_specs=[whole((rows, out)), whole((rows, out)), whole((2, out))]
                + [whole((layers, out))] * 4
                + [weight_spec, wide_params[0]],
                out_specs=[whole((rows, out)), columns(2, WIDE), whole((1, out)), whole((1, out))],
                out_shape=[jax.ShapeDtypeStruct((rows, out), jnp.bfloat16), f32(2, mid), f32(1, out), f32(1, out)],
                compiler_params=PARAMS,
            )(current, projected, out_sums, out_mean, out_var, out_gain, out_bias, expand_weight, mid_mean)
            out_means.append(new_mean)
            out_vars.append(new_var)
        sums = all_sum(stats, n_row, n_col, 1)
        spread, stats, mean_a, var_a = pl.pallas_call(
            functools.partial(spread_kernel, side, batch, row_count, blocks),
            grid=(wide_steps,),
            in_specs=[whole((rows, out)), weight_spec, layer_columns(taps_count, WIDE, layer), columns(2, WIDE)]
            + wide_params,
            out_specs=[
                pl.BlockSpec((2, rows, LANES), lambda j: (j, 0, 0)),
                columns(2, WIDE), columns(1, WIDE), columns(1, WIDE),
            ],
            out_shape=[f32(2 * wide_steps, rows, LANES), f32(2, mid), f32(1, mid), f32(1, mid)],
            scratch_shapes=[
                pltpu.VMEM((2, side, side, batch, LANES), jnp.float32),
                pltpu.VMEM((taps_count, 8, LANES), jnp.float32),
            ],
            compiler_params=PARAMS,
        )(current, expand_weight, depth_kernel, sums, mid_mean, mid_var, mid_gain, mid_bias)
        sums = all_sum(stats, n_row, n_col, 1)
        projected, stats, mean_b, var_b = pl.pallas_call(
            functools.partial(lift_kernel, layer, side, batch, row_count, mid),
            grid=(blocks,),
            in_specs=[pl.BlockSpec((1, rows, LANES), lambda j: (j, 0, 0)), columns(2, LANES)]
            + [layer_columns(2, LANES, layer)] * 4
            + [
                of_layer(squeeze_weight.shape, layer), whole(squeeze_bias.shape),
                of_layer(excite_weight.shape, layer), whole(excite_bias.shape),
                of_layer(project_weight.shape, layer), whole(out_mean.shape),
            ],
            out_specs=[whole((rows, out)), whole((2, out)), columns(1, LANES), columns(1, LANES)],
            out_shape=[f32(rows, out), f32(2, out), f32(1, mid), f32(1, mid)],
            scratch_shapes=[
                pltpu.VMEM((blocks, rows, LANES), jnp.float32),
                pltpu.VMEM((batch, blocks * LANES), jnp.float32),
                pltpu.VMEM((batch, blocks * LANES), jnp.float32),
                pltpu.VMEM((chunk, mid), jnp.bfloat16),
            ],
            compiler_params=PARAMS,
        )(
            spread, sums, mid_mean, mid_var, mid_gain, mid_bias,
            squeeze_weight, squeeze_bias, excite_weight, excite_bias, project_weight, out_mean,
        )
        out_sums = all_sum(stats, n_row, n_col, 2)
        means += [mean_a, mean_b]
        variances += [var_a, var_b]
    last = layers - 1
    scale, shift, new_mean, new_var = coefficients(
        out_sums[0], out_sums[1], row_count, out_mean[last], out_var[last], out_gain[last], out_bias[last]
    )
    out_means.append(new_mean[None])
    out_vars.append(new_var[None])
    current = (current.astype(jnp.float32) + projected * scale + shift).astype(jnp.bfloat16)
    current = current.reshape(side * side, batch, out).transpose(1, 0, 2).reshape(images.shape)
    return (
        current,
        jnp.concatenate(means).reshape(mid_mean.shape),
        jnp.concatenate(variances).reshape(mid_var.shape),
        jnp.concatenate(out_means),
        jnp.concatenate(out_vars),
    )


def solution(mesh):
    images_spec = P(("row", "col"), None, None, None)
    return jax.shard_map(
        functools.partial(per_device, mesh.shape["row"], mesh.shape["col"]),
        mesh=mesh,
        in_specs=(images_spec,) + (P(),) * 15,
        out_specs=(images_spec, P(), P(), P(), P()),
        check_vma=False,
    )
```

```python
import functools

import jax
import jax.numpy as jnp
from jax import lax
from jax.experimental import pallas as pl
from jax.experimental.pallas import tpu as pltpu
from jax.sharding import PartitionSpec as P

KERN = 5
REACH = KERN // 2
LANES = 128
WIDE = 2 * LANES
SLOTS = 3
TRANSPOSED = (((1,), (1,)), ((), ()))

EPSILON = 0.001
RATIO_MAX = 3.0
SHIFT_MAX = 5.0
MOMENTUM = 0.01

VMEM_BYTES = 60 * 1024 * 1024


def coefficients(first_sum, second_sum, row_count, run_mean, run_var, gain, bias):
    offset = first_sum / row_count
    batch_var = second_sum / row_count - offset * offset
    batch_mean = run_mean + offset
    batch_sigma = jnp.sqrt(batch_var + EPSILON)
    run_sigma = jnp.sqrt(run_var + EPSILON)
    scale_ratio = jnp.clip(batch_sigma / run_sigma, 1.0 / RATIO_MAX, RATIO_MAX)
    shift_clip = jnp.clip(offset / run_sigma, -SHIFT_MAX, SHIFT_MAX)
    gain_scale = gain * scale_ratio / batch_sigma
    gain_shift = bias + gain * shift_clip - batch_mean * gain_scale
    new_mean = run_mean + MOMENTUM * offset
    new_var = run_var + MOMENTUM * (batch_var - run_var)
    return (gain_scale, gain_shift, new_mean, new_var)


def half_silu(half_value):
    return half_value + half_value * jnp.tanh(half_value)


def fold_rows(values):
    return jnp.sum(values.reshape(-1, 8, values.shape[-1]), axis=0)


def exchange_kernel(n_row, n_col, x_ref, o_ref, buf_row, part, buf_col, s_row, r_row, s_col, r_col):
    row = lax.axis_index("row")
    col = lax.axis_index("col")
    row_peers = [lax.rem(row + k, n_row) for k in range(1, n_row)]
    col_peers = [lax.rem(col + k, n_col) for k in range(1, n_col)]
    mesh_id = pl.DeviceIdType.MESH
    barrier = pltpu.get_barrier_semaphore()
    for peer in row_peers:
        pl.semaphore_signal(barrier, inc=1, device_id=(peer, col), device_id_type=mesh_id)
    for peer in col_peers:
        pl.semaphore_signal(barrier, inc=1, device_id=(row, peer), device_id_type=mesh_id)
    pl.semaphore_wait(barrier, len(row_peers) + len(col_peers))

    copies = []
    for k, peer in enumerate(row_peers):
        copy = pltpu.make_async_remote_copy(
            src_ref=x_ref,
            dst_ref=buf_row.at[row],
            send_sem=s_row.at[k],
            recv_sem=r_row.at[k],
            device_id=(peer, col),
            device_id_type=mesh_id,
        )
        copy.start()
        copies.append(copy)
    buf_row[row] = x_ref[...]
    for copy in copies:
        copy.wait()
    total = buf_row[0]
    for k in range(1, n_row):
        total = total + buf_row[k]
    part[...] = total
    copies = []
    for k, peer in enumerate(col_peers):
        copy = pltpu.make_async_remote_copy(
            src_ref=part,
            dst_ref=buf_col.at[col],
            send_sem=s_col.at[k],
            recv_sem=r_col.at[k],
            device_id=(row, peer),
            device_id_type=mesh_id,
        )
        copy.start()
        copies.append(copy)
    buf_col[col] = total
    for copy in copies:
        copy.wait()
    total = buf_col[0]
    for k in range(1, n_col):
        total = total + buf_col[k]
    o_ref[...] = total


def all_sum(stats, n_row, n_col, collective_id):
    shape = stats.shape
    vmem = pl.BlockSpec(memory_space=pltpu.VMEM)
    return pl.pallas_call(
        functools.partial(exchange_kernel, n_row, n_col),
        out_shape=jax.ShapeDtypeStruct(shape, jnp.float32),
        in_specs=[vmem],
        out_specs=vmem,
        scratch_shapes=[
            pltpu.VMEM((n_row,) + shape, jnp.float32),
            pltpu.VMEM(shape, jnp.float32),
            pltpu.VMEM((n_col,) + shape, jnp.float32),
            pltpu.SemaphoreType.DMA((n_row - 1,)),
            pltpu.SemaphoreType.DMA((n_row - 1,)),
            pltpu.SemaphoreType.DMA((n_col - 1,)),
            pltpu.SemaphoreType.DMA((n_col - 1,)),
        ],
        compiler_params=pltpu.CompilerParams(collective_id=collective_id, has_side_effects=True),
    )(stats)


def expand_stats_kernel(layer, chunk, x_ref, w_ref, mean_ref, stats_ref):
    mid = w_ref.shape[2]
    for start in range(0, mid, WIDE):
        stop = min(mid, start + WIDE)
        mean = mean_ref[layer, 0:1, start:stop]

        def body(step, carry):
            rows = pl.ds(pl.multiple_of(step * chunk, chunk), chunk)
            y = jnp.dot(x_ref[rows, :], w_ref[0, :, start:stop], preferred_element_type=jnp.float32)
            centered = y - mean
            return carry[0] + fold_rows(centered), carry[1] + fold_rows(centered * centered)

        zero = jnp.zeros((8, stop - start), jnp.float32)
        first, second = lax.fori_loop(0, x_ref.shape[0] // chunk, body, (zero, zero), unroll=4)
        stats_ref[0:1, start:stop] = jnp.sum(first, axis=0, keepdims=True)
        stats_ref[1:2, start:stop] = jnp.sum(second, axis=0, keepdims=True)


def residual_kernel(
    layer, chunk, row_count, x_ref, p_ref, s_ref, m_ref, v_ref, g_ref, b_ref, w_ref, mean_ref,
    cur_ref, stats_ref, nm_ref, nv_ref,
):
    pick = slice(layer - 1, layer)
    scale, shift, new_mean, new_var = coefficients(
        s_ref[0:1, :], s_ref[1:2, :], row_count,
        m_ref[pick, :], v_ref[pick, :], g_ref[pick, :], b_ref[pick, :],
    )
    nm_ref[...] = new_mean
    nv_ref[...] = new_var

    def body(step, carry):
        rows = pl.ds(pl.multiple_of(step * chunk, chunk), chunk)
        cur_ref[rows, :] = (
            x_ref[rows, :].astype(jnp.float32) + p_ref[rows, :] * scale + shift
        ).astype(jnp.bfloat16)
        return carry

    lax.fori_loop(0, x_ref.shape[0] // chunk, body, 0, unroll=2)
    expand_stats_kernel(layer, chunk, cur_ref, w_ref, mean_ref, stats_ref)


def spread_kernel(
    layer, side, batch, row_count, blocks, x_ref, w_ref, dk_ref, sums_ref, mean_ref, var_ref, gain_ref, bias_ref,
    spread_ref, stats_ref, nm_ref, nv_ref, act, taps,
):
    chunk = side * batch
    scale, shift, new_mean, new_var = coefficients(
        sums_ref[0:1, :], sums_ref[1:2, :], row_count,
        mean_ref[0, 0:1, :], var_ref[0, 0:1, :], gain_ref[0, 0:1, :], bias_ref[0, 0:1, :],
    )
    nm_ref[...] = new_mean
    nv_ref[...] = new_var
    half_scale, half_shift = 0.5 * scale, 0.5 * shift
    weight = w_ref[0]

    def activate(step, carry):
        rows = pl.ds(pl.multiple_of(step * chunk, chunk), chunk)
        y = jnp.dot(x_ref[rows, :], weight, preferred_element_type=jnp.float32)
        active = half_silu(y * half_scale + half_shift).astype(jnp.bfloat16).astype(jnp.float32)
        for half in range(2):
            act[half, step] = active[:, half * LANES : (half + 1) * LANES].reshape(side, batch, LANES)
        return carry

    lax.fori_loop(0, side, activate, 0, unroll=4)

    def half_block(half, carry):
        lanes = pl.ds(pl.multiple_of(half * LANES, LANES), LANES)
        for tap in range(KERN * KERN):
            taps[tap] = jnp.broadcast_to(dk_ref[tap, layer : layer + 1, lanes], (8, LANES))
        mean = jnp.broadcast_to(mean_ref[0, 1:2, lanes], (8, LANES))

        def row(h, steps, sums):
            first, second = sums
            for sub in range(batch // 8):
                total = [None] * side
                for dy in steps:
                    line = [act[half, h + dy - REACH, w, sub * 8 : sub * 8 + 8, :] for w in range(side)]
                    for dx in range(KERN):
                        tap = taps[dy * KERN + dx]
                        for w in range(side):
                            source = w + dx - REACH
                            if 0 <= source < side:
                                term = line[source] * tap
                                total[w] = term if total[w] is None else total[w] + term
                for w in range(side):
                    start = pl.multiple_of((h * side + w) * batch + sub * 8, 8)
                    spread_ref[half, pl.ds(start, 8), :] = total[w]
                    centered = total[w] - mean
                    first = first + centered
                    second = second + centered * centered
            return first, second

        zero = jnp.zeros((8, LANES), jnp.float32)
        sums = (zero, zero)
        for h in range(REACH):
            sums = row(h, range(REACH - h, KERN), sums)
        sums = lax.fori_loop(REACH, side - REACH, lambda h, c: row(h, range(KERN), c), sums)
        for h in range(side - REACH, side):
            sums = row(h, range(0, side - h + REACH), sums)
        stats_ref[0:1, lanes] = jnp.sum(sums[0], axis=0, keepdims=True)
        stats_ref[1:2, lanes] = jnp.sum(sums[1], axis=0, keepdims=True)
        return carry

    halves = jnp.minimum(2, blocks - 2 * pl.program_id(0))
    lax.fori_loop(0, halves, half_block, 0)


def lift_kernel(
    layer, side, batch, row_count, mid, v_ref, sums_ref, mean_ref, var_ref, gain_ref, bias_ref,
    sw_ref, sb_ref, ew_ref, eb_ref, pw_ref, om_ref, proj_ref, stats_ref, nm_ref, nv_ref,
    lifted, pooled, gate, scaled,
):
    chunk = side * batch
    block = pl.program_id(0)
    blocks = pl.num_programs(0)
    scale, shift, new_mean, new_var = coefficients(
        sums_ref[0:1, :], sums_ref[1:2, :], row_count,
        mean_ref[0, 1:2, :], var_ref[0, 1:2, :], gain_ref[0, 1:2, :], bias_ref[0, 1:2, :],
    )
    nm_ref[...] = new_mean
    nv_ref[...] = new_var
    half_scale, half_shift = 0.5 * scale, 0.5 * shift

    for half in range(2):
        lanes = slice(half * LANES, (half + 1) * LANES)

        def lift(step, total):
            rows = pl.ds(pl.multiple_of(step * chunk, chunk), chunk)
            value = half_silu(v_ref[half, rows, :] * half_scale[:, lanes] + half_shift[:, lanes])
            lifted[2 * block + half, rows, :] = value
            return total + jnp.sum(value.reshape(side, batch, LANES), axis=0)

        total = lax.fori_loop(0, side, lift, jnp.zeros((batch, LANES), jnp.float32), unroll=4)
        start = pl.multiple_of((2 * block + half) * LANES, LANES)
        pooled[:, pl.ds(start, LANES)] = total / float(side * side)

    @pl.when(block == blocks - 1)
    def _():
        pick = slice(layer, layer + 1)
        squeezed = lax.dot_general(
            pooled[:, :mid], sw_ref[:, layer, :], TRANSPOSED,
            precision=lax.Precision.HIGHEST, preferred_element_type=jnp.float32,
        )
        squeezed = half_silu(0.5 * (squeezed + sb_ref[pick, :]))
        grown = jnp.dot(
            squeezed, ew_ref[:, layer, :], precision=lax.Precision.HIGHEST, preferred_element_type=jnp.float32
        )
        gate[:, :mid] = 0.5 + 0.5 * jnp.tanh(0.5 * (grown + eb_ref[pick, :]))
        out_mean = om_ref[pick, :]

        def project(step, slot, sums):
            rows = pl.ds(pl.multiple_of(step * chunk, chunk), chunk)
            for index in range(pl.cdiv(mid, LANES)):
                start = index * LANES
                stop = min(mid, start + LANES)
                value = lifted[index, rows, :].reshape(side, batch, LANES) * gate[:, start : start + LANES]
                value = value.astype(jnp.bfloat16).reshape(chunk, LANES)
                scaled[slot, :, start:stop] = value[:, : stop - start]
            product = lax.dot_general(
                scaled[slot], pw_ref[0], TRANSPOSED, preferred_element_type=jnp.float32
            )
            proj_ref[rows, :] = product
            centered = product - out_mean
            return sums[0] + fold_rows(centered), sums[1] + fold_rows(centered * centered)

        def project_group(group, sums):
            for slot in range(SLOTS):
                sums = project(group * SLOTS + slot, slot, sums)
            return sums

        zero = jnp.zeros((8, proj_ref.shape[1]), jnp.float32)
        first, second = lax.fori_loop(0, side // SLOTS, project_group, (zero, zero))
        stats_ref[0:1, :] = jnp.sum(first, axis=0, keepdims=True)
        stats_ref[1:2, :] = jnp.sum(second, axis=0, keepdims=True)


def whole(shape):
    return pl.BlockSpec(shape, lambda j: (0,) * len(shape))


def of_layer(shape, layer):
    return pl.BlockSpec((1,) + shape[1:], lambda j: (layer,) + (0,) * (len(shape) - 1))


def columns(rows, width):
    return pl.BlockSpec((rows, width), lambda j: (0, j))


def layer_columns(rows, width, layer):
    return pl.BlockSpec((1, rows, width), lambda j: (layer, 0, j))


def f32(*shape):
    return jax.ShapeDtypeStruct(shape, jnp.float32)


PARAMS = pltpu.CompilerParams(vmem_limit_bytes=VMEM_BYTES, dimension_semantics=("arbitrary",))


def per_device(n_row, n_col, *args):
    (
        images, expand_weight, depth_kernel, squeeze_weight, squeeze_bias, excite_weight, excite_bias,
        project_weight, mid_gain, mid_bias, out_gain, out_bias, mid_mean, mid_var, out_mean, out_var,
    ) = args
    batch, side, _, out = images.shape
    layers, _, mid = expand_weight.shape
    squeeze = squeeze_weight.shape[2]
    rows = side * side * batch
    chunk = side * batch
    row_count = float(rows * n_row * n_col)
    wide_steps = pl.cdiv(mid, WIDE)
    blocks = pl.cdiv(mid, LANES)
    taps_count = depth_kernel.shape[1]

    current = images.reshape(batch, side * side, out).transpose(1, 0, 2).reshape(rows, out)
    projected = None
    out_sums = None
    means, variances, out_means, out_vars = [], [], [], []
    for layer in range(layers):
        wide_params = [layer_columns(2, WIDE, layer)] * 4
        depth_spec = pl.BlockSpec((taps_count, layers, WIDE), lambda j: (0, 0, j))
        weight_spec = layer_columns(out, WIDE, layer)
        if layer == 0:
            stats = pl.pallas_call(
                functools.partial(expand_stats_kernel, layer, chunk),
                grid=(1,),
                in_specs=[whole((rows, out)), of_layer(expand_weight.shape, layer), whole(mid_mean.shape)],
                out_specs=whole((2, mid)),
                out_shape=f32(2, mid),
                compiler_params=PARAMS,
            )(current, expand_weight, mid_mean)
        else:
            current, stats, new_mean, new_var = pl.pallas_call(
                functools.partial(residual_kernel, layer, chunk, row_count),
                grid=(1,),
                in_specs=[whole((rows, out)), whole((rows, out)), whole((2, out))]
                + [whole((layers, out))] * 4
                + [of_layer(expand_weight.shape, layer), whole(mid_mean.shape)],
                out_specs=[whole((rows, out)), whole((2, mid)), whole((1, out)), whole((1, out))],
                out_shape=[jax.ShapeDtypeStruct((rows, out), jnp.bfloat16), f32(2, mid), f32(1, out), f32(1, out)],
                compiler_params=PARAMS,
            )(current, projected, out_sums, out_mean, out_var, out_gain, out_bias, expand_weight, mid_mean)
            out_means.append(new_mean)
            out_vars.append(new_var)
        sums = all_sum(stats, n_row, n_col, 1)
        spread, stats, mean_a, var_a = pl.pallas_call(
            functools.partial(spread_kernel, layer, side, batch, row_count, blocks),
            grid=(wide_steps,),
            in_specs=[whole((rows, out)), weight_spec, depth_spec, columns(2, WIDE)]
            + wide_params,
            out_specs=[
                pl.BlockSpec((2, rows, LANES), lambda j: (j, 0, 0)),
                columns(2, WIDE), columns(1, WIDE), columns(1, WIDE),
            ],
            out_shape=[f32(2 * wide_steps, rows, LANES), f32(2, mid), f32(1, mid), f32(1, mid)],
            scratch_shapes=[
                pltpu.VMEM((2, side, side, batch, LANES), jnp.float32),
                pltpu.VMEM((taps_count, 8, LANES), jnp.float32),
            ],
            compiler_params=PARAMS,
        )(current, expand_weight, depth_kernel.transpose(1, 0, 2), sums, mid_mean, mid_var, mid_gain, mid_bias)
        sums = all_sum(stats, n_row, n_col, 1)
        projected, stats, mean_b, var_b = pl.pallas_call(
            functools.partial(lift_kernel, layer, side, batch, row_count, mid),
            grid=(wide_steps,),
            in_specs=[pl.BlockSpec((2, rows, LANES), lambda j: (j, 0, 0)), columns(2, WIDE)]
            + wide_params
            + [
                whole((squeeze, layers, mid)), whole(squeeze_bias.shape),
                whole((squeeze, layers, mid)), whole(excite_bias.shape),
                of_layer((layers, out, mid), layer), whole(out_mean.shape),
            ],
            out_specs=[whole((rows, out)), whole((2, out)), columns(1, WIDE), columns(1, WIDE)],
            out_shape=[f32(rows, out), f32(2, out), f32(1, mid), f32(1, mid)],
            scratch_shapes=[
                pltpu.VMEM((2 * wide_steps, rows, LANES), jnp.float32),
                pltpu.VMEM((batch, wide_steps * WIDE), jnp.float32),
                pltpu.VMEM((batch, wide_steps * WIDE), jnp.float32),
                pltpu.VMEM((SLOTS, chunk, mid), jnp.bfloat16),
            ],
            compiler_params=PARAMS,
        )(
            spread, sums, mid_mean, mid_var, mid_gain, mid_bias,
            squeeze_weight.transpose(2, 0, 1), squeeze_bias, excite_weight.transpose(1, 0, 2), excite_bias,
            project_weight.transpose(0, 2, 1), out_mean,
        )
        out_sums = all_sum(stats, n_row, n_col, 2)
        means += [mean_a, mean_b]
        variances += [var_a, var_b]
    last = layers - 1
    scale, shift, new_mean, new_var = coefficients(
        out_sums[0], out_sums[1], row_count, out_mean[last], out_var[last], out_gain[last], out_bias[last]
    )
    out_means.append(new_mean[None])
    out_vars.append(new_var[None])
    current = (current.astype(jnp.float32) + projected * scale + shift).astype(jnp.bfloat16)
    current = current.reshape(side * side, batch, out).transpose(1, 0, 2).reshape(images.shape)
    return (
        current,
        jnp.concatenate(means).reshape(mid_mean.shape),
        jnp.concatenate(variances).reshape(mid_var.shape),
        jnp.concatenate(out_means),
        jnp.concatenate(out_vars),
    )


def solution(mesh):
    images_spec = P(("row", "col"), None, None, None)
    return jax.shard_map(
        functools.partial(per_device, mesh.shape["row"], mesh.shape["col"]),
        mesh=mesh,
        in_specs=(images_spec,) + (P(),) * 15,
        out_specs=(images_spec, P(), P(), P(), P()),
        check_vma=False,
    )
```
